32 devices in a mesh: group: 4 (over y, core), sub: 8 (over z, x).
Axes of the slice: x: 2, y: 2, z: 4, core: 2. Of those that a mesh axis runs over, the one named last changes fastest.
Arguments:
- shared_sizes: int32 [4, 8, 2], P('group', 'sub'), may hold values from 0 to 256, as said below
- stiffness: float32 [4, 8], P('group', 'sub'), may hold values from 0.1 to 10
- load_cases: float32 [4, 8, 1024, 384], P('group', 'sub'), may hold values from -6 to 6
- schur_blocks: bfloat16 [4, 8, 1024, 1024], P('group', 'sub')
- neumann_inverse: bfloat16 [4, 8, 1024, 1024], P('group', 'sub')
- coarse_basis: bfloat16 [4, 8, 32, 1024], P('group', 'sub'), may hold values from -0.1875 to 0.1875
- coarse_dofs: int32 [4, 8, 32], P('group', 'sub'), may hold values from 0 to 511
- coarse_inverse: float32 [512, 512], P('sub'), as said below
Outputs:
- solution: float32 [4, 8, 1024, 384], P('group', 'sub')
- residual: float32 [4, 8, 1024, 384], P('group', 'sub')
The draws below stay inside these ranges and needn't reach their ends.
Inputs may be any that keep to these rules, and one draw needn't show every extreme that they name: shared_sizes[g, s, 0] equals shared_sizes[g, s - 1, 1]; the lower share of the first and the upper share of the last subdomain of a group are 0, the other shares lie in 128 to 256, and in every group some subdomain shares exactly 256 with its upper neighbour. `coarse_inverse`: symmetric.
All inputs are finite; a program needn't handle non-finite values.
Results may differ from the reference program's by a relative error of at most 0.0075.
Values sent between devices are 32-bit elements; how exact they have to be, the bound alone decides.
No kernel may reach another device: no remote copies, remote signals or barrier semaphores. Data moves between devices by JAX's collectives and lax.ppermute only.
A program may use at most 128 MiB of HBM per device.

```python
import math
import jax
import jax.numpy as jnp
from jax import lax

NI = 1024
CASES = 384
MAXSH = 256
NCL = 32
ITERS = 4
NC = 512
N_GROUP = 4
N_SUB = 8


def operator_pair(key):
    key_diag, key_off = jax.random.split(jax.random.fold_in(key, 11))
    diagonal = jax.random.uniform(key_diag, (N_GROUP, N_SUB, NI), jnp.float32, 0.8, 1.6)
    perturb = jax.random.normal(key_off, (N_GROUP, N_SUB, NI, NI), jnp.float32) * (0.25 / math.sqrt(NI))
    perturb = (perturb + jnp.swapaxes(perturb, 2, 3)) * (1.0 / math.sqrt(2.0))
    identity = jnp.eye(NI, dtype=jnp.float32)
    inverse = 1.0 / diagonal
    schur = diagonal[..., :, None] * identity + perturb
    neumann = inverse[..., :, None] * identity - inverse[..., :, None] * perturb * inverse[..., None, :]
    return (schur, neumann)


def draw_schur_blocks(key, part):
    return operator_pair(key)[0].astype(jnp.bfloat16)


def draw_neumann_inverse(key, part):
    return operator_pair(key)[1].astype(jnp.bfloat16)


def draw_shared_sizes(key, part):
    key_size, key_peak = jax.random.split(jax.random.fold_in(key, 23))
    upper = jax.random.randint(key_size, (N_GROUP, N_SUB), MAXSH // 2, MAXSH + 1)
    peak_at = jax.random.randint(key_peak, (N_GROUP, 1), 0, N_SUB - 1)
    position = jnp.arange(N_SUB)[None, :]
    upper = jnp.where(position == peak_at, MAXSH, upper)
    upper = jnp.where(position == N_SUB - 1, 0, upper)
    lower = jnp.concatenate([jnp.zeros((N_GROUP, 1), upper.dtype), upper[:, :-1]], axis=1)
    return jnp.stack([lower, upper], axis=-1).astype(jnp.int32)


def draw_coarse_inverse(key, part):
    perturb = jax.random.normal(jax.random.fold_in(key, 37), (NC, NC), jnp.float32) * (0.25 / math.sqrt(NC))
    perturb = (perturb + perturb.T) * (1.0 / math.sqrt(2.0))
    return jnp.eye(NC, dtype=jnp.float32) + perturb


def plant(array, stream_key, low, top_value):
    index_at = [jax.random.randint(jax.random.fold_in(stream_key, axis), (), 0, length) for axis, length in enumerate(array.shape)]
    widest = array.shape.index(max(array.shape))
    neighbour = index_at[:widest] + [(index_at[widest] + 1) % array.shape[widest]] + index_at[widest + 1:]
    return array.at[tuple(index_at)].set(low).at[tuple(neighbour)].set(top_value)


def level_of(rng, extent, cuts, smallest, high):
    gain, own = 1.0, jax.random.fold_in(rng, 6)
    for dim, parts in cuts:
        heights = jnp.exp(jax.random.uniform(jax.random.fold_in(own, dim), (parts,), jnp.float32, smallest / len(cuts), high / len(cuts)))
        gain = gain * jnp.repeat(heights, extent[dim] // parts).reshape([-1 if axis == dim else 1 for axis in range(len(extent))])
    return gain


def centred(key, shape, width, bound, cuts=(), held_as=jnp.bfloat16):
    drawn = width * jax.random.normal(key, shape, jnp.float32)
    if cuts:
        drawn = drawn * level_of(key, shape, cuts, -0.22, 0.18)
    return jnp.clip(drawn, -bound, bound).astype(held_as)


def setup_inputs(seed: int = 0) -> dict:
    splits = jax.random.split(jax.random.key(seed), 9)
    return {
        "shared_sizes": draw_shared_sizes(jax.random.fold_in(splits[8], 71), 0),
        "stiffness": jnp.clip(jnp.exp(math.log(10.0) - 4.6051702 * jax.random.uniform(splits[1], (N_GROUP, N_SUB), jnp.float32) ** level_of(splits[1], (N_GROUP, N_SUB), ((0, 4), (1, 8)), -0.2, 0.2)), 0.1, 10.0),
        "load_cases": centred(splits[2], (N_GROUP, N_SUB, NI, CASES), 1.0, 6.0, ((0, 4), (1, 8)), jnp.float32),
        "schur_blocks": draw_schur_blocks(jax.random.fold_in(splits[8], 71), 0),
        "neumann_inverse": draw_neumann_inverse(jax.random.fold_in(splits[8], 71), 0),
        "coarse_basis": centred(splits[5], (N_GROUP, N_SUB, NCL, NI), (NI ** -0.5), 0.1875, ((0, 4), (1, 8))),
        "coarse_dofs": plant(jax.random.randint(splits[6], (N_GROUP, N_SUB, NCL), 0, NC), jax.random.fold_in(splits[6], 1), 0, NC - 1).astype(jnp.int32),
        "coarse_inverse": draw_coarse_inverse(jax.random.fold_in(splits[8], 71), 0),
    }


OMEGA = 0.6


def lift_piece(tail_rows, share_size):
    slab_width = tail_rows.shape[0]
    rolled = jnp.roll(tail_rows, share_size - slab_width, axis=0)
    inside = (jnp.arange(slab_width) < share_size)[:, None]
    return jnp.where(inside, rolled, jnp.zeros_like(rolled))


def place_piece(head_rows, share_size):
    slab_width = head_rows.shape[0]
    inside = (jnp.arange(slab_width) < share_size)[:, None]
    masked = jnp.where(inside, head_rows, jnp.zeros_like(head_rows))
    return jnp.roll(masked, slab_width - share_size, axis=0)


def assemble(vector, shared_sizes):
    tail_rows = vector[:, :, NI - MAXSH:]
    head_rows = vector[:, :, :MAXSH]
    lifted = jax.vmap(jax.vmap(lift_piece))(tail_rows, shared_sizes[:, :, 1])
    from_lower = jnp.concatenate([jnp.zeros_like(lifted[:, :1]), lifted[:, :-1]], axis=1)
    from_upper = jnp.concatenate([head_rows[:, 1:], jnp.zeros_like(head_rows[:, :1])], axis=1)
    placed = jax.vmap(jax.vmap(place_piece))(from_upper, shared_sizes[:, :, 1])
    return jnp.concatenate([head_rows + from_lower, vector[:, :, MAXSH:NI - MAXSH], tail_rows + placed], axis=2)


def interface_weights(shared_sizes, stiffness):
    nothing = jnp.zeros_like(stiffness[:, :1])
    lower = jnp.concatenate([nothing, stiffness[:, :-1]], axis=1)
    upper = jnp.concatenate([stiffness[:, 1:], nothing], axis=1)
    low_weight = stiffness / (stiffness + lower)
    up_weight = stiffness / (stiffness + upper)
    row_index = jnp.arange(NI)[None, None, :]
    ones_like = jnp.ones((1, 1, NI), jnp.float32)
    chosen = jnp.where(row_index >= NI - shared_sizes[:, :, 1:2], up_weight[..., None], ones_like)
    chosen = jnp.where(row_index < shared_sizes[:, :, 0:1], low_weight[..., None], chosen)
    return chosen[..., None]


def batched_dot(matrices, vectors):
    def one_pair(pair):
        return jnp.dot(pair[0], pair[1], preferred_element_type=jnp.float32)
    return lax.map(one_pair, (matrices, vectors))


def reference(shared_sizes, stiffness, load_cases, schur_blocks, neumann_inverse, coarse_basis, coarse_dofs, coarse_inverse):
    groups, subs = stiffness.shape
    count = groups * subs
    cases = load_cases.shape[-1]
    order = coarse_inverse.shape[0]
    weight = interface_weights(shared_sizes, stiffness)
    schur_flat = schur_blocks.reshape(count, NI, NI)
    neumann_flat = neumann_inverse.reshape(count, NI, NI)
    basis32 = coarse_basis.astype(jnp.float32)
    dof_flat = coarse_dofs.reshape(-1).astype(jnp.int32)

    def operator_residual(solution):
        product = batched_dot(schur_flat, solution.astype(jnp.bfloat16).reshape(count, NI, cases))
        return load_cases - product.reshape(groups, subs, NI, cases)

    solution = jnp.zeros((groups, subs, NI, cases), jnp.float32)
    for sweep in range(ITERS):
        local = operator_residual(solution)
        weighted = (weight * assemble(local, shared_sizes)).astype(jnp.bfloat16)
        terms = jnp.einsum('gsji,gsib->gsjb', basis32, weighted.astype(jnp.float32))
        gathered = jnp.zeros((order, cases), jnp.float32).at[dof_flat].add(terms.reshape(-1, cases))
        solved = jnp.dot(coarse_inverse, gathered, precision=lax.Precision.HIGHEST)
        picked = solved[coarse_dofs].astype(jnp.bfloat16)
        correction = batched_dot(neumann_flat, weighted.reshape(count, NI, cases)).reshape(groups, subs, NI, cases)
        correction = correction + jnp.einsum('gsji,gsjb->gsib', basis32, picked.astype(jnp.float32))
        solution = solution + OMEGA * assemble(weight * correction, shared_sizes)
    residual = assemble(operator_residual(solution), shared_sizes)
    return solution, residual
```

```python
import jax
import jax.numpy as jnp
from jax import lax
from jax.sharding import PartitionSpec as P

MAXSH = 256
ITERS = 4
OMEGA = 0.6
HIGHEST = lax.Precision.HIGHEST
EVERYONE = ("group", "sub")


def from_behind(block, axis, distance):
    devices = range(lax.axis_size(axis))
    route = [(i - distance, i) for i in devices if i - distance in devices]
    return lax.ppermute(block, axis, route)


def exchange(to_upper, to_lower):
    return from_behind(to_upper, "sub", 1), from_behind(to_lower, "sub", -1)


def bf16_dot(a, b):
    return jnp.dot(a, b, preferred_element_type=jnp.float32)


def exact_dot(a, b):
    return jnp.dot(a, b, precision=HIGHEST)


def replicate_rows(block, axis):
    peers = lax.axis_size(axis)
    copies = jnp.broadcast_to(block[None], (peers, *block.shape))
    return lax.all_to_all(copies, axis, split_axis=0, concat_axis=0, tiled=True)


def on_device(
    shared_sizes,
    stiffness,
    load_cases,
    schur_blocks,
    neumann_inverse,
    coarse_basis,
    coarse_dofs,
    coarse_inverse,
):
    groups, subs = lax.axis_size("group"), lax.axis_size("sub")
    peers = groups * subs
    share_low = shared_sizes[0, 0, 0]
    share_up = shared_sizes[0, 0, 1]
    loads = load_cases[0, 0]
    schur = schur_blocks[0, 0]
    neumann = neumann_inverse[0, 0]
    basis = coarse_basis[0, 0]
    unknowns, cases = loads.shape
    slots = basis.shape[0]
    order = coarse_inverse.shape[1]
    own_cases = cases // peers
    tail = unknowns - MAXSH

    row = jnp.arange(MAXSH)
    lift = (row[None, :] == row[:, None] + (MAXSH - share_up)).astype(jnp.bfloat16)
    lower = (row[None, :] == row[:, None] - (MAXSH - share_low)).astype(jnp.bfloat16)

    def both_ways(matrix):
        return bf16_dot(lift, matrix[tail:]).astype(matrix.dtype), bf16_dot(lower, matrix[:MAXSH]).astype(matrix.dtype)

    load_up = exact_dot(lift.astype(jnp.float32), loads[tail:])
    load_low = exact_dot(lower.astype(jnp.float32), loads[:MAXSH])

    own_stiff = stiffness[0, 0]
    coefficient = jnp.full((8, MAXSH), own_stiff, jnp.float32)
    basis_up = lax.dot_general(basis[:, tail:], lift, (((1,), (1,)), ((), ())), preferred_element_type=jnp.float32)
    basis_low = lax.dot_general(basis[:, :MAXSH], lower, (((1,), (1,)), ((), ())), preferred_element_type=jnp.float32)
    from_low, from_up = exchange(
        jnp.concatenate([basis_up, coefficient], axis=0), jnp.concatenate([basis_low, coefficient], axis=0)
    )
    low_stiff, up_stiff = from_low[slots, 0], from_up[slots, 0]
    low_weight = own_stiff / (own_stiff + low_stiff)
    up_weight = own_stiff / (own_stiff + up_stiff)
    lows_weight = low_stiff / (own_stiff + low_stiff)
    ups_weight = up_stiff / (own_stiff + up_stiff)
    row_index = jnp.arange(unknowns)
    weight = jnp.where(
        row_index < share_low,
        low_weight,
        jnp.where(row_index >= unknowns - share_up, up_weight, jnp.float32(1.0)),
    )
    near_basis = jnp.concatenate(
        [
            basis.astype(jnp.float32) * weight[None, :],
            jnp.pad(from_up[:slots] * ups_weight, ((0, 0), (tail, 0))),
            jnp.pad(from_low[:slots] * lows_weight, ((0, 0), (0, tail))),
        ],
        axis=0,
    )
    near = near_basis.shape[0]
    weight = weight[:, None]

    neumann_up, neumann_low = both_ways(neumann)
    schur_up, schur_low = both_ways(schur)

    part = coarse_inverse.shape[0] // groups
    mine = lax.dynamic_slice_in_dim(coarse_inverse, lax.axis_index("group") * part, part, axis=0)
    inverse = replicate_rows(mine, "sub")
    inverse = replicate_rows(inverse, "group").reshape(groups, subs, part, order)
    inverse = inverse.transpose(1, 0, 2, 3).reshape(order, order)
    dofs = replicate_rows(jnp.pad(coarse_dofs[0, 0].astype(jnp.float32), (0, 128 - slots)), EVERYONE)[:, :slots]
    near_dofs = jnp.concatenate([dofs, jnp.roll(dofs, -1, axis=0), jnp.roll(dofs, 1, axis=0)], axis=1)
    place = (near_dofs.reshape(-1)[:, None] == jnp.arange(order, dtype=jnp.float32)[None, :]).astype(jnp.bfloat16)

    def coarse(local):
        terms = exact_dot(near_basis, local)
        terms = terms.reshape(near, peers, own_cases).transpose(1, 2, 0).reshape(peers, own_cases * near)
        all_terms = lax.all_to_all(terms, EVERYONE, split_axis=0, concat_axis=0, tiled=True)
        all_terms = all_terms.reshape(peers, own_cases, near).transpose(1, 0, 2).reshape(own_cases, peers * near)
        gathered = exact_dot(all_terms, place.astype(jnp.float32))
        solved = exact_dot(gathered, inverse)
        picked = lax.dot_general(
            solved.astype(jnp.bfloat16), place, (((1,), (1,)), ((), ())), preferred_element_type=jnp.float32
        )
        picked = picked.reshape(own_cases, peers, near).transpose(1, 0, 2).reshape(peers, own_cases * near)
        picked = lax.all_to_all(picked, EVERYONE, split_axis=0, concat_axis=0, tiled=True)
        picked = picked.reshape(cases, near)
        return lax.dot_general(near_basis, picked, (((0,), (1,)), ((), ())), precision=HIGHEST)

    def assembled(own, low, up):
        return jnp.concatenate([own[:MAXSH] + low, own[MAXSH:tail], own[tail:] + up], axis=0)

    solution = jnp.zeros((unknowns, cases), jnp.float32)
    local, local_up, local_low = loads, load_up, load_low
    for sweep in range(ITERS):
        low, up = exchange(local_up, local_low)
        coarse_part = coarse(local)
        weighted = (weight * assembled(local, low, up)).astype(jnp.bfloat16)
        low, up = exchange(up_weight * bf16_dot(neumann_up, weighted), low_weight * bf16_dot(neumann_low, weighted))
        own = weight * bf16_dot(neumann, weighted) + coarse_part
        solution = solution + OMEGA * assembled(own, low, up)
        rounded = solution.astype(jnp.bfloat16)
        local_up = load_up - bf16_dot(schur_up, rounded)
        local_low = load_low - bf16_dot(schur_low, rounded)
        local = loads - bf16_dot(schur, rounded)
    low, up = exchange(local_up, local_low)
    residual = assembled(local, low, up)
    return (solution[None, None], residual[None, None])


def solution(mesh):
    return jax.shard_map(
        on_device,
        mesh=mesh,
        in_specs=(
            P("group", "sub", None),
            P("group", "sub"),
            P("group", "sub", None, None),
            P("group", "sub", None, None),
            P("group", "sub", None, None),
            P("group", "sub", None, None),
            P("group", "sub", None),
            P("sub", None),
        ),
        out_specs=(P("group", "sub", None, None), P("group", "sub", None, None)),
        check_vma=False,
    )
```

```python
import functools

import jax
import jax.numpy as jnp
from jax import lax
from jax.experimental import pallas as pl
from jax.experimental.pallas import tpu as pltpu
from jax.sharding import PartitionSpec as P

MAXSH = 256
ITERS = 4
OMEGA = 0.6
LANES = 128
HIGHEST = lax.Precision.HIGHEST
EVERYONE = ("group", "sub")
COARSE_IN_VMEM = 4 * 2**20


def swap(block, axis, partner_of):
    peers = range(lax.axis_size(axis))
    route = [(i, partner_of(i)) for i in peers if partner_of(i) in peers]
    return lax.ppermute(block, axis, route)


def near_partner(i):
    return i ^ 1


def far_partner(i):
    return ((i + 1) ^ 1) - 1


def exchange(near_slab, far_slab):
    near = swap(near_slab, "sub", near_partner)
    far = swap(far_slab, "sub", far_partner)
    return near, far


def bf16_dot(a, b):
    return jnp.dot(a, b, preferred_element_type=jnp.float32)


def contract(a, b, dims):
    return lax.dot_general(a, b, (dims, ((), ())), preferred_element_type=jnp.float32)


def exact_dot(a, b):
    return jnp.dot(a, b, precision=HIGHEST)


def halves(x):
    high = x.astype(jnp.bfloat16)
    return high, (x - high.astype(jnp.float32)).astype(jnp.bfloat16)


def across(weight, width):
    return jnp.concatenate([weight] * (width // LANES), axis=1)


def f32(*shape):
    return jax.ShapeDtypeStruct(shape, jnp.float32)


def bf16(*shape):
    return jax.ShapeDtypeStruct(shape, jnp.bfloat16)


SCALARS = pl.BlockSpec(memory_space=pltpu.SMEM)
VECTORS = pl.BlockSpec(memory_space=pltpu.VMEM)


def call(kernel, outs, *operands, scratch=(), flops=10**9):
    return pl.pallas_call(
        kernel,
        out_shape=outs,
        in_specs=[SCALARS if x.ndim == 1 else VECTORS for x in operands],
        out_specs=jax.tree.map(lambda _: VECTORS, outs),
        scratch_shapes=scratch,
        compiler_params=pltpu.CompilerParams(vmem_limit_bytes=20 * 2**20),
        cost_estimate=pl.CostEstimate(flops=flops, bytes_accessed=0, transcendentals=0),
    )(*operands)


def ends(head, tail):
    odd = lax.axis_index("sub") % 2 == 1
    return jnp.where(odd, head, tail), jnp.where(odd, tail, head)


def selections(facts):
    lift = MAXSH - facts[1]
    lower = facts[0] - MAXSH
    near_shift, far_shift = ends(lower, lift)
    distance = lax.broadcasted_iota(jnp.int32, (MAXSH, MAXSH), 1) - lax.broadcasted_iota(
        jnp.int32, (MAXSH, MAXSH), 0
    )
    near = (distance == near_shift).astype(jnp.float32).astype(jnp.bfloat16)
    far = (distance == far_shift).astype(jnp.float32).astype(jnp.bfloat16)
    return near, far


def info_kernel(facts, stiff, basis, near_info, far_info):
    slots = basis.shape[0]
    tail = basis.shape[1] - MAXSH
    near, far = selections(facts)
    both = ends(basis[:, 0:MAXSH].astype(jnp.float32), basis[:, tail:].astype(jnp.float32))
    for pick, source, out in zip((near, far), both, (near_info, far_info)):
        out[0:slots] = contract(source.astype(jnp.bfloat16), pick, ((1,), (1,)))
        out[slots:] = jnp.full((8, MAXSH), stiff[0], jnp.float32)


def prepare_kernel(facts, loads, near_load, far_load):
    tail = loads.shape[0] - MAXSH
    near, far = selections(facts)
    for pick, source, out in zip((near, far), ends(loads[0:MAXSH], loads[tail:]), (near_load, far_load)):
        high, _ = halves(source)
        middle, low = halves(source - high.astype(jnp.float32))
        out[...] = bf16_dot(pick, high) + (bf16_dot(pick, middle) + bf16_dot(pick, low))


def shift_kernel(facts, neumann, schur, neumann_shifted, schur_shifted):
    tail = neumann.shape[0] - MAXSH
    near, far = selections(facts)
    for matrix, out in ((neumann, neumann_shifted), (schur, schur_shifted)):
        sources = ends(matrix[0:MAXSH].astype(jnp.float32), matrix[tail:].astype(jnp.float32))
        out[0:MAXSH] = bf16_dot(near, sources[0].astype(jnp.bfloat16)).astype(jnp.bfloat16)
        out[MAXSH:] = bf16_dot(far, sources[1].astype(jnp.bfloat16)).astype(jnp.bfloat16)


def weights_kernel(facts, stiff, near_info, far_info, basis, weight, pair, near_basis, spread):
    slots, unknowns = basis.shape
    tail = unknowns - MAXSH
    own = stiff[0]
    near_stiff = near_info[slots:, 0:LANES]
    far_stiff = far_info[slots:, 0:LANES]
    near_weight, far_weight = own / (own + near_stiff), own / (own + far_stiff)
    pair[0:8], pair[8:] = near_weight, far_weight
    low_weight, up_weight = ends(near_weight, far_weight)
    low_weight, up_weight = low_weight[0:1], up_weight[0:1]

    def weight_at(index, low, up):
        return jnp.where(index < facts[0], low, jnp.where(index >= unknowns - facts[1], up, 1.0))

    index = lax.broadcasted_iota(jnp.int32, (unknowns, LANES), 0)
    weight[...] = weight_at(index, low_weight, up_weight)
    index = lax.broadcasted_iota(jnp.int32, (slots, unknowns), 1)
    repeat = unknowns // LANES
    own_rows = basis[...].astype(jnp.float32) * weight_at(
        index, jnp.concatenate([low_weight] * repeat, axis=1), jnp.concatenate([up_weight] * repeat, axis=1)
    )
    weighted = []
    for info, other in ((near_info, near_stiff), (far_info, far_stiff)):
        share = (other / (own + other))[0:1]
        weighted.append(info[0:slots] * jnp.concatenate([share] * (MAXSH // LANES), axis=1))
    low_rows, up_rows = ends(*weighted)
    gap = jnp.zeros((slots, tail), jnp.float32)
    rest = jnp.zeros((LANES - 3 * slots, unknowns), jnp.float32)
    everything = jnp.concatenate(
        [
            own_rows,
            jnp.concatenate([gap, up_rows], axis=1),
            jnp.concatenate([low_rows, gap], axis=1),
            rest,
        ],
        axis=0,
    )
    near_basis[0:LANES], near_basis[LANES:] = halves(everything)
    spread[:, 0:LANES], spread[:, LANES:] = halves(everything.T)


def thirds(unknowns):
    return slice(0, MAXSH), slice(MAXSH, unknowns - MAXSH), slice(unknowns - MAXSH, unknowns)


FIRST, SECOND = slice(0, MAXSH), slice(MAXSH, 2 * MAXSH)


def local_kernel(first, last, loads, *refs):
    refs = list(refs)
    unknowns = loads.shape[0]
    head, middle, tail = thirds(unknowns)
    if first:
        local = loads
    else:
        schur, inner, outer = refs[:3]
        refs = refs[3:]
    if last:
        (local, rounded) = refs
    else:
        near_basis, dofs, weight, shifted, ends_out, weighted, total, terms = refs[:8]
        if not first:
            local, rounded = refs[8:]
    if not first:
        rounded[head] = outer[FIRST]
        rounded[middle] = inner[...]
        rounded[tail] = outer[SECOND]

        @pl.loop(0, unknowns // MAXSH)
        def _(i):
            at = pl.ds(pl.multiple_of(i * MAXSH, MAXSH), MAXSH)
            local[at] = loads[at] - bf16_dot(schur[at], rounded[...])

    if last:
        return
    width = loads.shape[1]
    ends_out[FIRST] = local[head]
    ends_out[SECOND] = local[tail]
    weighted[...] = (across(weight[middle], width) * local[middle]).astype(jnp.bfloat16)
    total[...] = bf16_dot(shifted[:, middle], weighted[...])
    high, low = halves(local[...])
    both = bf16_dot(near_basis[...], high)
    done = (both[0:LANES] + both[LANES:] + bf16_dot(near_basis[0:LANES], low)).T
    peers, held = terms.shape[:2]
    count = width // peers
    for p in range(peers):
        terms[p, 0:count] = done[p * count : (p + 1) * count]
        terms[p, count:] = jnp.broadcast_to(dofs[...], (held - count, LANES))


def local_part(loads, schur, rounded, coarse_side, weight, shifted, peers, last):
    unknowns, cases = loads.shape
    first = schur is None
    inside = unknowns - 2 * MAXSH
    held = -(-(cases // peers + 1) // 8) * 8
    operands = [loads] if first else [loads, schur, *rounded]
    scratch = [pltpu.VMEM((unknowns, cases), jnp.float32), pltpu.VMEM((unknowns, cases), jnp.bfloat16)]
    if last:
        outs, scratch = f32(unknowns, cases), scratch[1:]
    else:
        operands += [*coarse_side, weight, shifted]
        outs = (
            f32(2 * MAXSH, cases), bf16(inside, cases), f32(2 * MAXSH, cases), f32(peers, held, LANES)
        )
        if first:
            scratch = []
    return call(functools.partial(local_kernel, first, last), outs, *operands, scratch=scratch)


def weigh_kernel(facts, local, near, far, weight, pair, shifted, total, weighted, near_slab, far_slab):
    unknowns, width = weight.shape[0], local.shape[1]
    head, _, tail = thirds(unknowns)
    low, up = ends(near[...], far[...])
    weighted[FIRST] = (across(weight[head], width) * (local[FIRST] + low)).astype(jnp.bfloat16)
    weighted[SECOND] = (across(weight[tail], width) * (local[SECOND] + up)).astype(jnp.bfloat16)
    for part, out, row in ((FIRST, near_slab, 0), (SECOND, far_slab, 8)):
        product = bf16_dot(shifted[part, head], weighted[FIRST]) + bf16_dot(shifted[part, tail], weighted[SECOND])
        out[...] = across(pair[row : row + 1], width) * (total[part] + product)


def weigh(facts, local, near, far, weight, pair, shifted, total):
    slab = f32(MAXSH, local.shape[1])
    outs = (bf16(*local.shape), slab, slab)
    return call(weigh_kernel, outs, facts, local, near, far, weight, pair, shifted, total)


def own_kernel(first, neumann, inner, outer, weight, picked, spread, shifted, near_load, far_load, *refs):
    refs = list(refs)
    unknowns, width = neumann.shape[0], inner.shape[1]
    head, middle, tail = thirds(unknowns)
    before = [None, None] if first else [refs.pop(0), refs.pop(0)]
    inner_out, rounded, outer_out, total, weighted = refs
    weighted[head] = outer[FIRST]
    weighted[middle] = inner[...]
    weighted[tail] = outer[SECOND]
    peers = picked.shape[0]
    count = width // peers
    values = jnp.concatenate([picked[p, 0:count] for p in range(peers)], axis=0).T.astype(jnp.bfloat16)
    values = jnp.concatenate([values, values], axis=0)

    def step(at, source, place):
        product = bf16_dot(neumann[at], weighted[...])
        change = OMEGA * (across(weight[at], width) * product + bf16_dot(spread[at], values))
        return change if first else source[place] + change

    outer_out[FIRST] = step(head, before[1], FIRST)
    outer_out[SECOND] = step(tail, before[1], SECOND)
    for start in range(0, inner.shape[0], MAXSH):
        place = slice(start, start + MAXSH)
        inside = step(slice(MAXSH + start, 2 * MAXSH + start), before[0], place)
        inner_out[place] = inside
        rounded[place] = inside.astype(jnp.bfloat16)
    total[FIRST] = near_load[...] - bf16_dot(shifted[FIRST, middle], rounded[...])
    total[SECOND] = far_load[...] - bf16_dot(shifted[SECOND, middle], rounded[...])


def own_part(neumann, inner, outer, weight, picked, spread, shifted, near_load, far_load, before):
    unknowns, width = neumann.shape[0], inner.shape[1]
    outs = (f32(*inner.shape), bf16(*inner.shape), f32(*outer.shape), f32(*outer.shape))
    return call(
        functools.partial(own_kernel, not before), outs,
        neumann, inner, outer, weight, picked, spread, shifted, near_load, far_load, *before,
        scratch=[pltpu.VMEM((unknowns, width), jnp.bfloat16)],
    )


def update_kernel(facts, outer, near, far, total, shifted, solution, rounded, near_slab, far_slab):
    unknowns = shifted.shape[1]
    head, _, tail = thirds(unknowns)
    low, up = ends(near[...], far[...])
    for part, extra in ((FIRST, low), (SECOND, up)):
        value = outer[part] + OMEGA * extra
        solution[part] = value
        rounded[part] = value.astype(jnp.bfloat16)
    for part, out in ((FIRST, near_slab), (SECOND, far_slab)):
        product = bf16_dot(shifted[part, head], rounded[FIRST]) + bf16_dot(shifted[part, tail], rounded[SECOND])
        out[...] = total[part] - product


def update(facts, outer, near, far, total, shifted):
    slab = f32(MAXSH, outer.shape[1])
    outs = (f32(*outer.shape), bf16(*outer.shape), slab, slab)
    return call(update_kernel, outs, facts, outer, near, far, total, shifted)


def final_kernel(local, near, far, residual):
    head, middle, tail = thirds(local.shape[0])
    low, up = ends(near[...], far[...])
    residual[head] = local[head] + low
    residual[middle] = local[middle]
    residual[tail] = local[tail] + up


def coarse_kernel(all_terms, place, inverse, picked):
    peers, held = all_terms.shape[:2]
    terms = jnp.concatenate([all_terms[p] for p in range(peers)], axis=1)
    gathered = bf16_dot(jnp.concatenate(halves(terms), axis=0), place[...])
    gathered = gathered[0:held] + gathered[held:]
    both = jnp.concatenate(halves(gathered), axis=0)
    order = gathered.shape[1]
    solved = bf16_dot(both, inverse[0:order])
    solved = solved[0:held] + solved[held:] + bf16_dot(both[0:held], inverse[order:])
    values = contract(solved.astype(jnp.bfloat16), place[...], ((1,), (1,)))
    for p in range(peers):
        picked[p] = values[:, p * LANES : (p + 1) * LANES]


def coarse(all_terms, place, inverse):
    if place.size > COARSE_IN_VMEM:
        peers, held = all_terms.shape[:2]
        terms = all_terms.transpose(1, 0, 2).reshape(held, peers * LANES)
        full = inverse[: place.shape[1]].astype(jnp.float32) + inverse[place.shape[1] :].astype(jnp.float32)
        solved = exact_dot(exact_dot(terms, place.astype(jnp.float32)), full)
        values = contract(solved.astype(jnp.bfloat16), place, ((1,), (1,)))
        return values.reshape(held, peers, LANES).transpose(1, 0, 2)
    return call(coarse_kernel, f32(*all_terms.shape), all_terms, place, inverse)


def gathered_inverse(block, groups, subs):
    part = block.shape[0] // groups
    held = lax.dynamic_slice_in_dim(block, lax.axis_index("group") * part, part, axis=0)[None]
    for axis, peers in (("sub", subs), ("group", groups)):
        bit = 1
        while bit < peers:
            other = swap(held, axis, lambda i: i ^ bit)
            held = jnp.concatenate([held, other], axis=0)
            bit *= 2
    j = jnp.arange(groups * subs)
    source = (lax.axis_index("sub") ^ (j % subs)) * groups + (lax.axis_index("group") ^ (j // subs))
    return held, source.astype(jnp.int32)


def sort_kernel(source, held, inverse):
    blocks, part, order = held.shape

    @pl.loop(0, blocks)
    def _(j):
        high, low = halves(held[j])
        at = pl.multiple_of(source[j] * part, part)
        inverse[pl.ds(at, part)] = high
        inverse[pl.ds(order + at, part)] = low


def on_device(
    shared_sizes,
    stiffness,
    load_cases,
    schur_blocks,
    neumann_inverse,
    coarse_basis,
    coarse_dofs,
    coarse_inverse,
):
    groups, subs = lax.axis_size("group"), lax.axis_size("sub")
    peers = groups * subs
    loads = load_cases[0, 0]
    schur = schur_blocks[0, 0]
    neumann = neumann_inverse[0, 0]
    basis = coarse_basis[0, 0]
    unknowns, cases = loads.shape
    slots = basis.shape[0]
    order = coarse_inverse.shape[1]
    facts = shared_sizes.reshape(2)
    stiff = stiffness.reshape(1)
    dofs = jnp.pad(coarse_dofs[0].astype(jnp.float32), ((0, 0), (0, LANES - slots)))

    slab, info = f32(MAXSH, cases), f32(slots + 8, MAXSH)
    near_info, far_info = call(info_kernel, (info, info), facts, stiff, basis)
    near_info, far_info = exchange(near_info, far_info)
    near_load, far_load = call(prepare_kernel, (slab, slab), facts, loads)
    near, far = exchange(near_load, far_load)
    held, source = gathered_inverse(coarse_inverse, groups, subs)
    out = bf16(2 * MAXSH, unknowns)
    neumann_shifted, schur_shifted = call(shift_kernel, (out, out), facts, neumann, schur)
    outs = (f32(unknowns, LANES), f32(16, LANES), bf16(2 * LANES, unknowns), bf16(unknowns, 2 * LANES))
    weight, pair, near_basis, spread = call(weights_kernel, outs, facts, stiff, near_info, far_info, basis)
    coarse_side = (near_basis, dofs)
    local, inner, total, terms = local_part(loads, None, None, coarse_side, weight, neumann_shifted, peers, False)
    if order % 16 == 0 and held.shape[1] % 16 == 0:
        out = bf16(2 * order, order)
        if order * order <= COARSE_IN_VMEM // 2:
            inverse = call(sort_kernel, out, source, held)
        else:
            inverse = jnp.zeros(held.shape, jnp.float32).at[source].set(held).reshape(order, order)
            inverse = jnp.concatenate(halves(inverse), axis=0)
    else:
        raise ValueError("part size")

    place = None
    before = ()
    for k in range(ITERS):
        last = k == ITERS - 1
        arrived = lax.all_to_all(terms, EVERYONE, split_axis=0, concat_axis=0, tiled=True)
        if k == 0:
            all_dofs = arrived[:, cases // peers, :slots]
            spare = jnp.full((peers, LANES - 3 * slots), -1.0, jnp.float32)
            around = [all_dofs, jnp.roll(all_dofs, -1, axis=0), jnp.roll(all_dofs, 1, axis=0), spare]
            around = jnp.concatenate(around, axis=1).reshape(-1)
            place = (around[:, None] == jnp.arange(order, dtype=jnp.float32)[None, :]).astype(jnp.bfloat16)
        solved = coarse(arrived, place, inverse)
        outer, near_slab, far_slab = weigh(facts, local, near, far, weight, pair, neumann_shifted, total)
        near, far = exchange(near_slab, far_slab)
        picked = lax.all_to_all(solved, EVERYONE, split_axis=0, concat_axis=0, tiled=True)
        inner, inner_rounded, outer, total = own_part(
            neumann, inner, outer, weight, picked, spread, schur_shifted, near_load, far_load, before
        )
        outer, outer_rounded, near_slab, far_slab = update(facts, outer, near, far, total, schur_shifted)
        before = (inner, outer)
        near, far = exchange(near_slab, far_slab)
        rounded = (inner_rounded, outer_rounded)
        done = local_part(loads, schur, rounded, coarse_side, weight, neumann_shifted, peers, last)
        if last:
            local = done
        else:
            local, inner, total, terms = done
    inner, outer = before
    state = jnp.concatenate([outer[FIRST], inner, outer[SECOND]], axis=0)
    residual = call(final_kernel, f32(unknowns, cases), local, near, far)
    return (state[None, None], residual[None, None])


def solution(mesh):
    return jax.shard_map(
        on_device,
        mesh=mesh,
        in_specs=(
            P("group", "sub", None),
            P("group", "sub"),
            P("group", "sub", None, None),
            P("group", "sub", None, None),
            P("group", "sub", None, None),
            P("group", "sub", None, None),
            P("group", "sub", None),
            P("sub", None),
        ),
        out_specs=(P("group", "sub", None, None), P("group", "sub", None, None)),
        check_vma=False,
    )
```
